32 devices in a mesh: pb: 4 (over y, core), ma: 8 (over z, x).
Axes of the slice: x: 2, y: 2, z: 4, core: 2. Of those that a mesh axis runs over, the one named last changes fastest.
Arguments:
- queries: bfloat16 [4096, 4096], P('pb', 'ma'), may hold values from -6 to 6
- keys: bfloat16 [2048, 4096], P('ma', 'pb'), may hold values from -6 to 6
- query_ids: int32 [4096], P('pb'), may hold values from 0 to 31999, as said below
- memory_ids: int32 [2048], P('ma'), may hold values from 0 to 31999, as said below
- target_gap: float32 [4096], P('pb'), may hold values from -4 to -0.5
- lse: float32 [4096], P('pb'), as said below
- counts: int32 [4096], P('pb'), may hold values from 1 to 8
Outputs:
- query_grad: float32 [4096, 4096], P('pb', 'ma')
- key_grad: float32 [2048, 4096], P('ma', 'pb')
The draws below stay inside these ranges and needn't reach their ends.
Inputs may be any that keep to these rules, and one draw needn't show every extreme that they name: query_ids and memory_ids are token ids drawn from one common frequency law, so that some query and memory rows share tokens. query_ids follow the same law as memory_ids. lse lies between log(2048) + 0.5 and log(2048) + 4.
All inputs are finite; a program needn't handle non-finite values.
Results may differ from the reference program's by a relative error of at most 0.0059.
Values may be sent and summed in bfloat16 or wider, within the bound.
No kernel may reach another device: no remote copies, remote signals or barrier semaphores. Data moves between devices by JAX's collectives and lax.ppermute only.
A program may use at most 64 MiB of HBM per device.

```python
import math
import jax
import jax.numpy as jnp
from jax import lax

D = 4096
VOCAB = 32000
GRAD_SCALE = 1024
NQ = 4096
NM = 2048


def token_table(key, which, length):
    order = jax.random.permutation(jax.random.fold_in(key, 7001), VOCAB)
    uniform_bits = jax.random.randint(jax.random.fold_in(key, which), (length,), 0, 2 ** 20)
    ranks = 2 ** 24 // (uniform_bits + 2 ** 10) - 16
    return order[ranks % VOCAB].astype(jnp.int32)


def draw_query_ids(key, part):
    return token_table(key, 11, NQ)


def draw_memory_ids(key, part):
    return token_table(key, 23, NM)


def draw_lse(key, part):
    inner = jax.random.fold_in(key, 31)
    spread = jax.random.uniform(inner, (NQ,), jnp.float32, 1.0, 3.0)
    return spread + jnp.log(jnp.float32(NM))


def set_ends(array, stream_key, smallest, largest):
    index_at = [jax.random.randint(jax.random.fold_in(stream_key, axis), (), 0, length) for axis, length in enumerate(array.shape)]
    longest = array.shape.index(max(array.shape))
    beside = index_at[:longest] + [(index_at[longest] + 1) % array.shape[longest]] + index_at[longest + 1:]
    return array.at[tuple(index_at)].set(smallest).at[tuple(beside)].set(largest)


def level_of(rng, dims, shards, least, top_value):
    def one(axis_at, parts):
        heights = jax.random.uniform(jax.random.fold_in(jax.random.fold_in(rng, 6), axis_at), (parts,), jnp.float32, least / len(shards), top_value / len(shards))
        return jnp.repeat(jnp.exp(heights), dims[axis_at] // parts).reshape((-1,) + (1,) * (len(dims) - axis_at - 1))

    gain = one(*shards[0])
    for cut in shards[1:]:
        gain = gain * one(*cut)
    return gain


def gaussian(own_key, shape, scale, limit, shards=(), held_as=jnp.bfloat16):
    drawn = scale * jax.random.normal(own_key, shape, jnp.float32)
    if shards:
        drawn = drawn * level_of(own_key, shape, shards, -0.22, 0.18)
    return jnp.clip(drawn, -limit, limit).astype(held_as)


def setup_inputs(seed: int = 0) -> dict:
    seeds = jax.random.split(jax.random.key(seed), 8)
    return {
        "queries": gaussian(seeds[0], (NQ, D), 1.0, 6.0, ((0, 4), (1, 8))),
        "keys": gaussian(seeds[1], (NM, D), 1.0, 6.0, ((0, 8), (1, 4))),
        "query_ids": draw_query_ids(jax.random.fold_in(seeds[7], 71), 0),
        "memory_ids": draw_memory_ids(jax.random.fold_in(seeds[7], 71), 0),
        "target_gap": jnp.clip(-4.0 + 3.5 * jax.random.uniform(seeds[4], (NQ,), jnp.float32) ** level_of(seeds[4], (NQ,), ((0, 4),), -0.2, 0.2), -4.0, -0.5),
        "lse": draw_lse(jax.random.fold_in(seeds[7], 71), 0),
        "counts": set_ends(jax.random.randint(seeds[6], (NQ,), 1, 9), jax.random.fold_in(seeds[6], 1), 1, 8).astype(jnp.int32),
    }


def reference(queries, keys, query_ids, memory_ids, target_gap, lse, counts):
    factor = 1.0 / math.sqrt(D)
    scores = jnp.dot(queries, keys.T, preferred_element_type=jnp.float32) * factor
    prob = jnp.exp(scores - lse[:, None])
    match = (query_ids[:, None] == memory_ids[None, :]).astype(jnp.float32)
    positive = jnp.exp(target_gap) + lax.optimization_barrier(jnp.sum(match * prob, axis=1))
    row_scale = jnp.float32(GRAD_SCALE) / counts.astype(jnp.float32)
    weight = ((prob - match * prob / positive[:, None]) * row_scale[:, None]).astype(jnp.bfloat16)
    query_grad = jnp.dot(weight, keys, preferred_element_type=jnp.float32) * factor
    key_grad = jnp.dot(weight.T, queries, preferred_element_type=jnp.float32) * factor
    return (query_grad, key_grad)
```

```python
import math

import jax
import jax.numpy as jnp
from jax import lax
from jax.sharding import PartitionSpec as P

GRAD_SCALE = 1024
CORES = 2
NZ = 4


def build(n_pb, n_ma):
    ny, nx = n_pb // CORES, n_ma // NZ
    axes = ("pb", "ma")

    def move(value, to):
        pairs = []
        for y in range(ny):
            for c in range(CORES):
                for z in range(NZ):
                    for x in range(nx):
                        ty, tc, tz, tx = to(y, c, z, x)
                        source = (y * CORES + c) * n_ma + z * nx + x
                        target = (ty * CORES + tc) * n_ma + tz * nx + tx
                        pairs.append((source, target))
        return lax.ppermute(value, axes, pairs)

    def to_sibling(value):
        return move(value, lambda y, c, z, x: (y, 1 - c, z, x))

    def over_y(value, step):
        return move(value, lambda y, c, z, x: ((y + step) % ny, c, z, x))

    def over_z(value, flip):
        return move(value, lambda y, c, z, x: (y, c, z ^ flip, x))

    def over_x(value, step):
        return move(value, lambda y, c, z, x: (y, c, z, (x + step) % nx))

    def on_device(queries, keys, query_ids, memory_ids, target_gap, lse, counts):
        pb, ma = lax.axis_index("pb"), lax.axis_index("ma")
        y, c = pb // CORES, pb % CORES
        z, x = ma // nx, ma % nx
        parity, half = z % 2, z // 2
        same = c == parity
        rows, feats = queries.shape
        mem, key_feats = keys.shape
        sub = rows // 2
        width = feats * n_ma
        factor = 1.0 / math.sqrt(width)

        def halves(value, axis):
            keep = lax.dynamic_slice_in_dim(value, c * sub, sub, axis)
            give = lax.dynamic_slice_in_dim(value, (1 - c) * sub, sub, axis)
            got = to_sibling(give)
            return jnp.where(same, keep, got), jnp.where(same, got, keep)

        mine, theirs = halves(queries, 0)
        by_z = {0: mine}
        for flip in (1, 2, 3):
            by_z[flip] = over_z(mine if flip == 2 else theirs, flip)
        q_full = jnp.zeros((sub, width), queries.dtype)
        for flip in (0, 1, 2, 3):
            for step in range(nx):
                piece = over_x(by_z[flip], step) if step else by_z[flip]
                at = (z ^ flip) * nx + (x - step) % nx
                q_full = lax.dynamic_update_slice_in_dim(q_full, piece, at * feats, 1)

        def pair_rows(own, other):
            low = jnp.where(parity == 0, own, other)
            high = jnp.where(parity == 0, other, own)
            return jnp.concatenate([low, high], axis=0)

        k_pair = pair_rows(keys, over_z(keys, 1))
        ids_pair = pair_rows(memory_ids, over_z(memory_ids, 1))
        k_full = jnp.zeros((2 * mem, width), keys.dtype)
        for step in range(ny):
            piece = over_y(k_pair, step) if step else k_pair
            at = ((y - step) % ny) * CORES
            k_full = lax.dynamic_update_slice_in_dim(k_full, piece, (at + c) * key_feats, 1)
            k_full = lax.dynamic_update_slice_in_dim(k_full, to_sibling(piece), (at + 1 - c) * key_feats, 1)

        mine_rows = lax.dynamic_slice_in_dim(k_full, c * mem, mem, 0)
        near = lax.dynamic_slice_in_dim(mine_rows, z * nx * feats, nx * feats, 1)
        far = over_z(lax.dynamic_slice_in_dim(mine_rows, (z ^ 2) * nx * feats, nx * feats, 1), 2)
        both = jnp.concatenate([near, far], axis=0)
        k_cols = []
        for step in range(nx):
            piece = lax.dynamic_slice_in_dim(both, ((x + step) % nx) * feats, feats, 1)
            piece = over_x(piece, step) if step else piece
            other = to_sibling(piece)
            first = jnp.where(c == 0, piece, other)
            second = jnp.where(c == 0, other, piece)
            k_cols.append([
                jnp.concatenate([first[:mem], second[:mem]], axis=0),
                jnp.concatenate([first[mem:], second[mem:]], axis=0),
            ])

        table = jnp.stack([
            query_ids.astype(jnp.float32),
            lse,
            jnp.exp(target_gap),
            jnp.float32(GRAD_SCALE) / counts.astype(jnp.float32),
        ])
        table, _ = halves(table, 1)
        ids_row, lse_row, gap_row, scale_row = (table[i][:, None] for i in range(4))

        scores = lax.dot_general(
            q_full, k_full, (((1,), (1,)), ((), ())), preferred_element_type=jnp.float32
        ) * factor
        prob = jnp.exp(scores - lse_row)
        match = (ids_row == ids_pair.astype(jnp.float32)[None, :]).astype(jnp.float32)
        part = jnp.sum(match * prob, axis=1)
        matched = part
        for step in range(1, nx):
            matched = matched + over_x(part, step)
        matched = matched + over_z(matched, 2)
        positive = gap_row + matched[:, None]
        weight = ((prob - match * prob / positive) * scale_row).astype(jnp.bfloat16)

        own_part = None
        received = []
        for step in list(range(1, ny)) + [0]:
            at = ((y + step) % ny) * CORES

            def partial(core):
                block = lax.dynamic_slice_in_dim(q_full, (at + core) * key_feats, key_feats, 1)
                return lax.dot_general(
                    weight, block, (((0,), (0,)), ((), ())), preferred_element_type=jnp.float32
                ) * factor

            got = to_sibling(partial(1 - c).astype(jnp.bfloat16))
            total = partial(c) + got.astype(jnp.float32)
            if step:
                received.append(over_y(total.astype(jnp.bfloat16), step))
            else:
                own_part = total
        for value in received:
            own_part = own_part + value.astype(jnp.float32)
        keep = lax.dynamic_slice_in_dim(own_part, parity * mem, mem, 0)
        give = lax.dynamic_slice_in_dim(own_part, (1 - parity) * mem, mem, 0).astype(jnp.bfloat16)
        key_grad = keep + over_z(give, 1).astype(jnp.float32)

        tiles = {0: weight}
        for flip in (1, 2, 3):
            tiles[flip] = over_z(weight, flip)
        grads = []
        for flips in ((0, 2), (1, 3)):
            left, right = [], []
            for far_half, flip in enumerate(flips):
                for step in range(nx):
                    left.append(over_x(tiles[flip], step) if step else tiles[flip])
                    right.append(k_cols[step][far_half])
            grads.append(
                jnp.dot(
                    jnp.concatenate(left, axis=1),
                    jnp.concatenate(right, axis=0),
                    preferred_element_type=jnp.float32,
                ) * factor
            )
        keep = jnp.where(same, grads[0], grads[1])
        got = to_sibling(jnp.where(same, grads[1], grads[0]))
        query_grad = jnp.concatenate(
            [jnp.where(c == 0, keep, got), jnp.where(c == 0, got, keep)], axis=0
        )
        return query_grad, key_grad

    return on_device


def solution(mesh):
    placed = (P("pb", "ma"), P("ma", "pb"), P("pb"), P("ma"), P("pb"), P("pb"), P("pb"))
    return jax.shard_map(
        build(mesh.shape["pb"], mesh.shape["ma"]),
        mesh=mesh,
        in_specs=placed,
        out_specs=(P("pb", "ma"), P("ma", "pb")),
        check_vma=False,
    )
```

```python
import math

import jax
import jax.numpy as jnp
from jax import lax
from jax.sharding import PartitionSpec as P


GRAD_SCALE = 1024
CORES = 2
NZ = 4
PARTS = 2


def build(n_pb, n_ma):
    ny, nx = n_pb // CORES, n_ma // NZ
    axes = ("pb", "ma")

    def move(value, to):
        pairs = []
        for y in range(ny):
            for c in range(CORES):
                for z in range(NZ):
                    for x in range(nx):
                        ty, tc, tz, tx = to(y, c, z, x)
                        source = (y * CORES + c) * n_ma + z * nx + x
                        target = (ty * CORES + tc) * n_ma + tz * nx + tx
                        pairs.append((source, target))
        return lax.ppermute(value, axes, pairs)

    def to_sibling(value):
        return move(value, lambda y, c, z, x: (y, 1 - c, z, x))

    def over_y(value, step):
        return move(value, lambda y, c, z, x: ((y + step) % ny, c, z, x))

    def over_z(value, flip):
        return move(value, lambda y, c, z, x: (y, c, z ^ flip, x))

    def over_x(value, step):
        return move(value, lambda y, c, z, x: (y, c, z, (x + step) % nx))

    def dot(a, b, dims):
        return lax.dot_general(a, b, (dims, ((), ())), preferred_element_type=jnp.float32)

    def on_device(queries, keys, query_ids, memory_ids, target_gap, lse, counts):
        pb, ma = lax.axis_index("pb"), lax.axis_index("ma")
        y, c = pb // CORES, pb % CORES
        z, x = ma // nx, ma % nx
        parity = z % 2
        same = c == parity
        rows, feats = queries.shape
        mem, key_feats = keys.shape
        sub = rows // 2
        width = feats * n_ma
        factor = 1.0 / math.sqrt(width)
        part_rows = sub // PARTS

        def cut(value, index, size, axis):
            return lax.dynamic_slice_in_dim(value, index * size, size, axis)

        def halves(value, axis):
            keep = cut(value, c, sub, axis)
            got = to_sibling(cut(value, 1 - c, sub, axis))
            return jnp.where(same, keep, got), jnp.where(same, got, keep)

        mine, theirs = halves(queries, 0)
        q_full = []
        for part in range(PARTS):
            at = slice(part * part_rows, (part + 1) * part_rows)
            by_z = {0: mine[at]}
            for flip in (1, 2, 3):
                by_z[flip] = over_z((mine if flip == 2 else theirs)[at], flip)
            whole = jnp.zeros((part_rows, width), queries.dtype)
            for flip in (0, 1, 2, 3):
                for step in range(nx):
                    piece = over_x(by_z[flip], step) if step else by_z[flip]
                    place = (z ^ flip) * nx + (x - step) % nx
                    whole = lax.dynamic_update_slice_in_dim(whole, piece, place * feats, 1)
            q_full.append(whole)

        def pair_rows(own, other):
            low = jnp.where(parity == 0, own, other)
            high = jnp.where(parity == 0, other, own)
            return jnp.concatenate([low, high], axis=0)

        k_pair = pair_rows(keys, over_z(keys, 1))
        ids_pair = pair_rows(memory_ids, over_z(memory_ids, 1)).astype(jnp.float32)
        k_full = jnp.zeros((2 * mem, width), keys.dtype)
        for step in range(ny):
            piece = over_y(k_pair, step) if step else k_pair
            at = ((y - step) % ny) * CORES
            k_full = lax.dynamic_update_slice_in_dim(k_full, piece, (at + c) * key_feats, 1)
            other = to_sibling(piece)
            k_full = lax.dynamic_update_slice_in_dim(k_full, other, (at + 1 - c) * key_feats, 1)

        span = nx * feats
        near = cut(k_full, z, span, 1)
        slab = mem // ny
        sent = cut(cut(k_full, c * ny + y, slab, 0), z ^ 2, span, 1)
        sent = over_z(sent, 2)
        far_own = jnp.zeros((mem, span), keys.dtype)
        for step in range(ny):
            piece = over_y(sent, step) if step else sent
            far_own = lax.dynamic_update_slice_in_dim(far_own, piece, ((y - step) % ny) * slab, 0)
        far_other = to_sibling(far_own)
        far = jnp.concatenate(
            [jnp.where(c == 0, far_own, far_other), jnp.where(c == 0, far_other, far_own)], axis=0
        )
        near, far = (
            jnp.concatenate([cut(v, (x + step) % nx, feats, 1) for step in range(nx)], axis=1)
            for v in (near, far)
        )

        table = jnp.stack([
            query_ids.astype(jnp.float32),
            lse,
            jnp.exp(target_gap),
            jnp.float32(GRAD_SCALE) / counts.astype(jnp.float32),
        ])
        table, _ = halves(table, 1)

        weights = []
        for part in range(PARTS):
            at = slice(part * part_rows, (part + 1) * part_rows)
            ids_row, lse_row, gap_row, scale_row = (table[i, at][:, None] for i in range(4))
            if part:
                q_full[part], _ = lax.optimization_barrier((q_full[part], weights[-1]))
            scores = dot(q_full[part], k_full, ((1,), (1,))) * factor
            prob = jnp.exp(scores - lse_row)
            match = (ids_row == ids_pair[None, :]).astype(jnp.float32)
            share = jnp.sum(match * prob, axis=1)
            matched = share
            for step in range(1, nx):
                matched = matched + over_x(share, step)
            matched = matched + over_z(matched, 2)
            positive = gap_row + matched[:, None]
            weights.append(((prob - match * prob / positive) * scale_row).astype(jnp.bfloat16))

        pieces = []
        for part in range(PARTS):
            tiles = {0: weights[part]}
            for flip in (1, 2, 3):
                tiles[flip] = over_z(weights[part], flip)
            grads = []
            for flips in ((0, 2), (1, 3)):
                total = (
                    dot(tiles[flips[0]], near, ((1,), (0,)))
                    + dot(tiles[flips[1]], far, ((1,), (0,)))
                ) * factor
                result = total[:, :feats]
                for step in range(1, nx):
                    sent = total[:, step * feats:(step + 1) * feats].astype(jnp.bfloat16)
                    got = over_x(sent, step)
                    result = result + got.astype(jnp.float32)
                grads.append(result)
            keep = jnp.where(same, grads[0], grads[1])
            got = to_sibling(jnp.where(same, grads[1], grads[0]))
            pieces.append((keep, got))
        first = [jnp.where(c == 0, keep, got) for keep, got in pieces]
        second = [jnp.where(c == 0, got, keep) for keep, got in pieces]
        query_grad = jnp.concatenate(first + second, axis=0)

        q_keep = [cut(v.reshape(-1, ny, CORES, key_feats), c, 1, 2).reshape(-1, ny * key_feats) for v in q_full]
        q_give = [cut(v.reshape(-1, ny, CORES, key_feats), 1 - c, 1, 2).reshape(-1, ny * key_feats) for v in q_full]

        def key_part(which):
            cols = [cut(w, which, mem, 1) for w in weights]
            give = sum(dot(w, q, ((0,), (0,))) for w, q in zip(cols, q_give)) * factor
            got = to_sibling(give.astype(jnp.bfloat16)).astype(jnp.float32)
            total = sum(dot(w, q, ((0,), (0,))) for w, q in zip(cols, q_keep)) * factor + got
            result = cut(total, y, key_feats, 1)
            for step in range(1, ny):
                sent = cut(total, (y + step) % ny, key_feats, 1).astype(jnp.bfloat16)
                result = result + over_y(sent, step).astype(jnp.float32)
            return result

        give = key_part(1 - parity).astype(jnp.bfloat16)
        key_grad = key_part(parity) + over_z(give, 1).astype(jnp.float32)
        return query_grad, key_grad

    return on_device


def solution(mesh):
    placed = (P("pb", "ma"), P("ma", "pb"), P("pb"), P("ma"), P("pb"), P("pb"), P("pb"))
    return jax.shard_map(
        build(mesh.shape["pb"], mesh.shape["ma"]),
        mesh=mesh,
        in_specs=placed,
        out_specs=(P("pb", "ma"), P("ma", "pb")),
        check_vma=False,
    )
```
